32 devices in a mesh: dp: 2 (over x), tp: 16 (over z, y, core).
Axes of the slice: x: 2, y: 2, z: 4, core: 2. Of those that a mesh axis runs over, the one named last changes fastest.
Arguments:
- hidden: bfloat16 [32, 12, 2560], P('dp'), parts along dimension 0
- norm_w: bfloat16 [2560], replicated
- embedding: bfloat16 [262144, 2560], P('tp')
- draft_ids: int32 [32, 12], P('dp'), parts along dimension 0
Outputs:
- output 1: float32 [32, 12], P('dp'), parts along dimension 0
- output 2: float32 [32, 12], P('dp'), parts along dimension 0
There are 2 independent parts. The reference program is written for one: setup_inputs(seed, part) draws one part's arguments, and reference() takes and returns one part's arrays. A program takes and returns all parts, laid end to end along the dimension named above; an argument that names none is the same for every part.
All inputs are finite; a program needn't handle non-finite values.
Results may differ from the reference program's by a relative error of at most 0.001.
Values sent between devices are 32-bit elements.
A program may use at most 1 GiB of HBM per device.

```python
import jax
import jax.numpy as jnp
from jax import lax

BATCH = 16
DRAFT = 12
D = 2560
VOCAB = 262144
EPS = 1e-6
ROW_BLOCK = 2 ** 11
HOT_IDS = VOCAB // 16
ALIGN_SCALE = 6.0
NOISE_SCALE = 3.0


def draw_embedding(key_coef, key_noise, direction):
    num_blocks = VOCAB // ROW_BLOCK

    def one_block(block_idx):
        tok_coef = jax.random.normal(jax.random.fold_in(key_coef, block_idx), (ROW_BLOCK, 1), jnp.float32)
        noise_rows = jax.random.normal(jax.random.fold_in(key_noise, block_idx), (ROW_BLOCK, D), jnp.float32)
        block_rows = ALIGN_SCALE * tok_coef * direction / D + NOISE_SCALE * noise_rows * D ** -0.5
        return block_rows.astype(jnp.bfloat16)

    return lax.map(one_block, jnp.arange(num_blocks)).reshape(VOCAB, D)


def setup_inputs(seed: int = 0, part: int = 0) -> dict:
    base_key = jax.random.key(seed)
    key_dir, key_w, key_coef, key_noise, key_part = jax.random.split(base_key, 5)
    key_part = jax.random.fold_in(key_part, part)
    key_mix, key_hid, key_pick, key_low, key_any = jax.random.split(key_part, 5)
    direction = jax.random.normal(key_dir, (D,), jnp.float32)
    mix_coef = jax.random.uniform(key_mix, (BATCH, DRAFT, 1), jnp.float32, -0.9, 0.9)
    hid_noise = jax.random.normal(key_hid, (BATCH, DRAFT, D), jnp.float32)
    hidden = mix_coef * direction + jnp.sqrt(1.0 - mix_coef * mix_coef) * hid_noise
    norm_w = 0.5 * jax.random.normal(key_w, (D,), jnp.float32)
    embedding = draw_embedding(key_coef, key_noise, direction)
    pick_kind = jax.random.randint(key_pick, (BATCH, DRAFT), 0, 4)
    low_ids = jax.random.randint(key_low, (BATCH, DRAFT), 0, HOT_IDS)
    any_ids = jax.random.randint(key_any, (BATCH, DRAFT), 0, VOCAB)
    draft_ids = jnp.where(pick_kind < 3, low_ids, any_ids).astype(jnp.int32)
    draft_ids = draft_ids.at[0, 0].set(VOCAB - 1).at[0, 1].set(0)
    return {"hidden": hidden.astype(jnp.bfloat16), "norm_w": norm_w.astype(jnp.bfloat16), "embedding": embedding, "draft_ids": draft_ids}


def reference(hidden, norm_w, embedding, draft_ids):
    gain = 1.0 + norm_w.astype(jnp.float32)

    def one_seq(seq_args):
        seq_hidden, seq_ids = seq_args
        x_float = seq_hidden.astype(jnp.float32)
        mean_sq = jnp.mean(x_float * x_float, axis=-1, keepdims=True)
        normed = (x_float * lax.rsqrt(mean_sq + EPS) * gain).astype(jnp.bfloat16)
        logits = jnp.dot(normed, embedding.T, preferred_element_type=jnp.float32)
        row_max = jnp.max(logits, axis=-1, keepdims=True)
        exp_shift = jnp.exp(logits - row_max)
        exp_total = jnp.sum(exp_shift, axis=-1)
        weighted = jnp.sum(exp_shift * logits, axis=-1)
        log_norm = row_max[:, 0] + jnp.log(exp_total)
        picked = jnp.take_along_axis(logits, seq_ids[:, None], axis=-1)[:, 0]
        return picked - log_norm, log_norm - weighted / exp_total

    log_prob, entropy = lax.map(one_seq, (hidden, draft_ids))
    return log_prob, entropy
```

```python
import functools

import jax
import jax.numpy as jnp
from jax import lax
from jax.experimental import pallas as pl
from jax.experimental.pallas import tpu as pltpu
from jax.sharding import PartitionSpec as P

EPS = 1e-6
LANES = 128
CHUNK = 512
SLOTS = 14
MESH = pl.DeviceIdType.MESH


def head_kernel(tp, x_hbm, w_ref, e_hbm, ids_ref, out_ref, x_buf, h_buf, e_buf, z_a, z_b,
                idp, m_ref, s_ref, a_ref, p_ref, stats, recv, x_sem, e_sem, send_sem, recv_sem):
    groups, batch, depth = x_hbm.shape
    tokens = groups * batch
    rows = e_hbm.shape[0]
    steps = rows // CHUNK
    width = h_buf.shape[0]
    me = lax.axis_index("tp")

    barrier = pltpu.get_barrier_semaphore()
    x_copy = pltpu.make_async_copy(x_hbm, x_buf, x_sem)
    x_copy.start()

    def e_copy(step, slot):
        first = pl.multiple_of(step * CHUNK, CHUNK)
        return pltpu.make_async_copy(e_hbm.at[pl.ds(first, CHUNK)], e_buf.at[slot], e_sem.at[slot])

    for slot in range(SLOTS):
        e_copy(slot, slot).start()
    for k in range(1, tp):
        pl.semaphore_signal(barrier, inc=1, device_id={"tp": lax.rem(me + k, tp)}, device_id_type=MESH)

    idp[...] = jnp.full_like(idp, -1)
    idp[0:batch, 0:groups] = ids_ref[...]
    by_group = jnp.transpose(idp[...])
    sub = lax.broadcasted_iota(jnp.int32, (8, LANES), 0)
    lane = lax.broadcasted_iota(jnp.int32, (8, LANES), 1)
    id_rows = []
    for half in range(width // LANES):
        part = pltpu.roll(by_group[8 * half:8 * half + 8], 0, 1, stride=batch, stride_axis=0)
        part = jnp.where(lane // batch == sub, part, 0)
        id_rows.append(jnp.sum(part, axis=0, keepdims=True))
    id_row = jnp.concatenate(id_rows, axis=1)
    sub_w = lax.broadcasted_iota(jnp.int32, (8, width), 0)
    lane_w = lax.broadcasted_iota(jnp.int32, (8, width), 1)
    wanted = jnp.where(lane_w < tokens, id_row - me * rows - sub_w, -(1 << 30))

    m_ref[...] = jnp.full_like(m_ref, -jnp.inf)
    s_ref[...] = jnp.zeros_like(s_ref)
    a_ref[...] = jnp.zeros_like(a_ref)
    p_ref[...] = jnp.zeros_like(p_ref)

    h_buf[tokens:width, :] = jnp.zeros((width - tokens, depth), h_buf.dtype)
    gain = 1.0 + w_ref[...].astype(jnp.float32)
    x_copy.wait()

    def norm(g, _):
        x = x_buf[g].astype(jnp.float32)
        mean_sq = jnp.sum(x * x, axis=-1, keepdims=True) * (1.0 / depth)
        normed = x * lax.rsqrt(mean_sq + EPS) * gain
        h_buf[pl.ds(pl.multiple_of(g * batch, batch), batch), :] = normed.astype(h_buf.dtype)
        return _

    lax.fori_loop(0, groups, norm, 0)

    def logits(slot):
        return lax.dot_general(e_buf[slot], h_buf[...], (((1,), (1,)), ((), ())),
                               preferred_element_type=jnp.float32)

    def fold(z_ref, step):
        z = z_ref[...].reshape(CHUNK // 8, 8, width)
        m_old = m_ref[...]
        m_new = jnp.maximum(m_old, jnp.max(z, axis=0))
        scale = jnp.exp(m_old - m_new)
        e = jnp.exp(z - m_new[None])
        m_ref[...] = m_new
        s_ref[...] = s_ref[...] * scale + jnp.sum(e, axis=0)
        a_ref[...] = a_ref[...] * scale + jnp.sum(e * z, axis=0)
        here = wanted - step * CHUNK
        at = 8 * lax.broadcasted_iota(jnp.int32, z.shape, 0)
        p_ref[...] += jnp.sum(jnp.where(here[None] == at, z, 0.0), axis=0)

    def one(step, into, other):
        slot = lax.rem(step, SLOTS)
        e_copy(step, slot).wait()
        into[...] = logits(slot)
        if other is not None:
            fold(other, step - 1)

        @pl.when(step + SLOTS < steps)
        def _():
            e_copy(step + SLOTS, slot).start()

    one(0, z_a, None)

    def pair(i, _):
        one(2 * i + 1, z_b, z_a)
        one(2 * i + 2, z_a, z_b)
        return _

    lax.fori_loop(0, (steps - 2) // 2, pair, 0)
    one(steps - 1, z_b, z_a)
    fold(z_b, steps - 1)

    m8 = m_ref[...]
    m1 = jnp.max(m8, axis=0, keepdims=True)
    c8 = jnp.exp(m8 - m1)
    s1 = jnp.sum(c8 * s_ref[...], axis=0, keepdims=True)
    a1 = jnp.sum(c8 * a_ref[...], axis=0, keepdims=True)
    p1 = jnp.sum(p_ref[...], axis=0, keepdims=True)
    own = jnp.concatenate([m1, s1, a1, p1], axis=0)
    stats[...] = own
    recv[me] = own

    pl.semaphore_wait(barrier, tp - 1)

    def send(k):
        peer = lax.rem(me + k, tp)
        return pltpu.make_async_remote_copy(
            src_ref=stats, dst_ref=recv.at[me], send_sem=send_sem.at[k], recv_sem=recv_sem.at[k],
            device_id={"tp": peer}, device_id_type=MESH)

    for k in range(1, tp):
        send(k).start()
    for k in range(1, tp):
        send(k).wait()

    r = recv[...]
    m = r[:, 0, :]
    top = jnp.max(m, axis=0, keepdims=True)
    c = jnp.exp(m - top)
    total = jnp.sum(c * r[:, 1, :], axis=0, keepdims=True)
    weighted = jnp.sum(c * r[:, 2, :], axis=0, keepdims=True)
    picked = jnp.sum(r[:, 3, :], axis=0, keepdims=True)
    log_norm = top + jnp.log(total)
    log_prob = picked - log_norm
    entropy = log_norm - weighted / total

    out = jnp.zeros((batch, LANES), jnp.float32)
    out_lane = lax.broadcasted_iota(jnp.int32, (batch, LANES), 1)
    row = lax.broadcasted_iota(jnp.int32, (LANES, LANES), 0)
    for half in range(width // LANES):
        cut = slice(half * LANES, (half + 1) * LANES)
        both = jnp.where(row < LANES // 2, log_prob[:, cut], entropy[:, cut])
        col = jnp.transpose(both)
        for j in range(LANES // batch):
            g = half * (LANES // batch) + j
            if g < groups:
                mine = (out_lane == g) | (out_lane == g + LANES // 2)
                out = jnp.where(mine, col[j * batch:(j + 1) * batch], out)
    out_ref[0] = out[:, 0:groups]
    out_ref[1] = out[:, LANES // 2:LANES // 2 + groups]


def solution(mesh):
    tp = mesh.shape["tp"]

    def local_part(hidden, norm_w, embedding, draft_ids):
        batch, groups, depth = hidden.shape
        width = pl.cdiv(batch * groups, 2 * LANES) * 2 * LANES
        x = jnp.transpose(hidden, (1, 0, 2))
        any_space = pl.BlockSpec(memory_space=pl.ANY)
        vmem = pl.BlockSpec(memory_space=pltpu.VMEM)
        out = pl.pallas_call(
            functools.partial(head_kernel, tp),
            out_shape=jax.ShapeDtypeStruct((2, batch, groups), jnp.float32),
            in_specs=[any_space, vmem, any_space, vmem],
            out_specs=vmem,
            scratch_shapes=[
                pltpu.VMEM((groups, batch, depth), hidden.dtype),
                pltpu.VMEM((width, depth), jnp.bfloat16),
                pltpu.VMEM((SLOTS, CHUNK, depth), embedding.dtype),
                pltpu.VMEM((CHUNK, width), jnp.float32),
                pltpu.VMEM((CHUNK, width), jnp.float32),
                pltpu.VMEM((LANES, LANES), jnp.int32),
                pltpu.VMEM((8, width), jnp.float32),
                pltpu.VMEM((8, width), jnp.float32),
                pltpu.VMEM((8, width), jnp.float32),
                pltpu.VMEM((8, width), jnp.float32),
                pltpu.VMEM((4, width), jnp.float32),
                pltpu.VMEM((tp, 4, width), jnp.float32),
                pltpu.SemaphoreType.DMA,
                pltpu.SemaphoreType.DMA((SLOTS,)),
                pltpu.SemaphoreType.DMA((tp,)),
                pltpu.SemaphoreType.DMA((tp,)),
            ],
            compiler_params=pltpu.CompilerParams(
                collective_id=0, has_side_effects=True, vmem_limit_bytes=60 * 1024 * 1024),
        )(x, norm_w.reshape(1, depth), embedding, draft_ids)
        return out[0], out[1]

    return jax.shard_map(
        local_part, mesh=mesh,
        in_specs=(P("dp", None, None), P(None), P("tp", None), P("dp", None)),
        out_specs=(P("dp", None), P("dp", None)), check_vma=False)
```

```python
import functools

import jax
import jax.numpy as jnp
from jax import lax
from jax.experimental import pallas as pl
from jax.experimental.pallas import tpu as pltpu
from jax.sharding import PartitionSpec as P

EPS = 1e-6
LANES = 128
CHUNK = 512
SLOTS = 4
MESH = pl.DeviceIdType.MESH


def head_kernel(tp, x_hbm, w_ref, e_hbm, ids_ref, out_ref, x_buf, h_buf, e_buf, z_a, z_b,
                idp, m_ref, s_ref, a_ref, p_ref, stats, recv, x_sem, e_sem, send_sem, recv_sem):
    groups, batch, depth = x_hbm.shape
    tokens = groups * batch
    rows = e_hbm.shape[0]
    steps = rows // CHUNK
    width = h_buf.shape[0]
    me = lax.axis_index("tp")

    barrier = pltpu.get_barrier_semaphore()
    x_copy = pltpu.make_async_copy(x_hbm, x_buf, x_sem)
    x_copy.start()

    def e_copy(step, slot):
        first = pl.multiple_of(step * CHUNK, CHUNK)
        return pltpu.make_async_copy(e_hbm.at[pl.ds(first, CHUNK)], e_buf.at[slot], e_sem.at[slot])

    for slot in range(SLOTS):
        e_copy(slot, slot).start()
    for k in range(1, tp):
        pl.semaphore_signal(barrier, inc=1, device_id={"tp": lax.rem(me + k, tp)}, device_id_type=MESH)

    idp[...] = jnp.full_like(idp, -1)
    idp[0:batch, 0:groups] = ids_ref[...]
    by_group = jnp.transpose(idp[...])
    sub = lax.broadcasted_iota(jnp.int32, (8, LANES), 0)
    lane = lax.broadcasted_iota(jnp.int32, (8, LANES), 1)
    id_rows = []
    for half in range(width // LANES):
        part = pltpu.roll(by_group[8 * half:8 * half + 8], 0, 1, stride=batch, stride_axis=0)
        part = jnp.where(lane // batch == sub, part, 0)
        id_rows.append(jnp.sum(part, axis=0, keepdims=True))
    id_row = jnp.concatenate(id_rows, axis=1)
    sub_w = lax.broadcasted_iota(jnp.int32, (8, width), 0)
    lane_w = lax.broadcasted_iota(jnp.int32, (8, width), 1)
    wanted = jnp.where(lane_w < tokens, id_row - me * rows - sub_w, -(1 << 30))

    m_ref[...] = jnp.full_like(m_ref, -jnp.inf)
    s_ref[...] = jnp.zeros_like(s_ref)
    a_ref[...] = jnp.zeros_like(a_ref)
    p_ref[...] = jnp.zeros_like(p_ref)

    h_buf[tokens:width, :] = jnp.zeros((width - tokens, depth), h_buf.dtype)
    gain = 1.0 + w_ref[...].astype(jnp.float32)
    x_copy.wait()

    def norm(g, _):
        x = x_buf[g].astype(jnp.float32)
        mean_sq = jnp.sum(x * x, axis=-1, keepdims=True) * (1.0 / depth)
        normed = x * lax.rsqrt(mean_sq + EPS) * gain
        h_buf[pl.ds(pl.multiple_of(g * batch, batch), batch), :] = normed.astype(h_buf.dtype)
        return _

    lax.fori_loop(0, groups, norm, 0)

    def logits(slot):
        return lax.dot_general(e_buf[slot], h_buf[...], (((1,), (1,)), ((), ())),
                               preferred_element_type=jnp.float32)

    def fold(z_ref, step):
        z = z_ref[...].reshape(CHUNK // 8, 8, width)
        m_old = m_ref[...]
        m_new = jnp.maximum(m_old, jnp.max(z, axis=0))
        scale = jnp.exp(m_old - m_new)
        e = jnp.exp(z - m_new[None])
        m_ref[...] = m_new
        s_ref[...] = s_ref[...] * scale + jnp.sum(e, axis=0)
        a_ref[...] = a_ref[...] * scale + jnp.sum(e * z, axis=0)
        here = wanted - step * CHUNK
        at = 8 * lax.broadcasted_iota(jnp.int32, z.shape, 0)
        p_ref[...] += jnp.sum(jnp.where(here[None] == at, z, 0.0), axis=0)

    def one(step, into, other):
        slot = lax.rem(step, SLOTS)
        e_copy(step, slot).wait()
        into[...] = logits(slot)
        if other is not None:
            fold(other, step - 1)

        @pl.when(step + SLOTS < steps)
        def _():
            e_copy(step + SLOTS, slot).start()

    one(0, z_a, None)

    def pair(i, _):
        one(2 * i + 1, z_b, z_a)
        one(2 * i + 2, z_a, z_b)
        return _

    lax.fori_loop(0, (steps - 2) // 2, pair, 0)
    one(steps - 1, z_b, z_a)
    fold(z_b, steps - 1)

    m8 = m_ref[...]
    m1 = jnp.max(m8, axis=0, keepdims=True)
    c8 = jnp.exp(m8 - m1)
    s1 = jnp.sum(c8 * s_ref[...], axis=0, keepdims=True)
    a1 = jnp.sum(c8 * a_ref[...], axis=0, keepdims=True)
    p1 = jnp.sum(p_ref[...], axis=0, keepdims=True)
    own = jnp.concatenate([m1, s1, a1, p1], axis=0)
    stats[...] = own
    recv[me] = own

    pl.semaphore_wait(barrier, tp - 1)

    def send(k):
        peer = lax.rem(me + k, tp)
        return pltpu.make_async_remote_copy(
            src_ref=stats, dst_ref=recv.at[me], send_sem=send_sem.at[k], recv_sem=recv_sem.at[k],
            device_id={"tp": peer}, device_id_type=MESH)

    for k in range(1, tp):
        send(k).start()
    for k in range(1, tp):
        send(k).wait()

    r = recv[...]
    m = r[:, 0, :]
    top = jnp.max(m, axis=0, keepdims=True)
    c = jnp.exp(m - top)
    total = jnp.sum(c * r[:, 1, :], axis=0, keepdims=True)
    weighted = jnp.sum(c * r[:, 2, :], axis=0, keepdims=True)
    picked = jnp.sum(r[:, 3, :], axis=0, keepdims=True)
    log_norm = top + jnp.log(total)
    log_prob = picked - log_norm
    entropy = log_norm - weighted / total

    out = jnp.zeros((batch, LANES), jnp.float32)
    out_lane = lax.broadcasted_iota(jnp.int32, (batch, LANES), 1)
    row = lax.broadcasted_iota(jnp.int32, (LANES, LANES), 0)
    for half in range(width // LANES):
        cut = slice(half * LANES, (half + 1) * LANES)
        both = jnp.where(row < LANES // 2, log_prob[:, cut], entropy[:, cut])
        col = jnp.transpose(both)
        for j in range(LANES // batch):
            g = half * (LANES // batch) + j
            if g < groups:
                mine = (out_lane == g) | (out_lane == g + LANES // 2)
                out = jnp.where(mine, col[j * batch:(j + 1) * batch], out)
    out_ref[0] = out[:, 0:groups]
    out_ref[1] = out[:, LANES // 2:LANES // 2 + groups]


def solution(mesh):
    tp = mesh.shape["tp"]

    def local_part(hidden, norm_w, embedding, draft_ids):
        batch, groups, depth = hidden.shape
        width = pl.cdiv(batch * groups, 2 * LANES) * 2 * LANES
        x = jnp.transpose(hidden, (1, 0, 2))
        any_space = pl.BlockSpec(memory_space=pl.ANY)
        vmem = pl.BlockSpec(memory_space=pltpu.VMEM)
        out = pl.pallas_call(
            functools.partial(head_kernel, tp),
            out_shape=jax.ShapeDtypeStruct((2, batch, groups), jnp.float32),
            in_specs=[any_space, vmem, any_space, vmem],
            out_specs=vmem,
            scratch_shapes=[
                pltpu.VMEM((groups, batch, depth), hidden.dtype),
                pltpu.VMEM((width, depth), jnp.bfloat16),
                pltpu.VMEM((SLOTS, CHUNK, depth), embedding.dtype),
                pltpu.VMEM((CHUNK, width), jnp.float32),
                pltpu.VMEM((CHUNK, width), jnp.float32),
                pltpu.VMEM((LANES, LANES), jnp.int32),
                pltpu.VMEM((8, width), jnp.float32),
                pltpu.VMEM((8, width), jnp.float32),
                pltpu.VMEM((8, width), jnp.float32),
                pltpu.VMEM((8, width), jnp.float32),
                pltpu.VMEM((4, width), jnp.float32),
                pltpu.VMEM((tp, 4, width), jnp.float32),
                pltpu.SemaphoreType.DMA,
                pltpu.SemaphoreType.DMA((SLOTS,)),
                pltpu.SemaphoreType.DMA((tp,)),
                pltpu.SemaphoreType.DMA((tp,)),
            ],
            compiler_params=pltpu.CompilerParams(
                collective_id=0, has_side_effects=True, vmem_limit_bytes=60 * 1024 * 1024),
        )(x, norm_w.reshape(1, depth), embedding, draft_ids)
        return out[0], out[1]

    return jax.shard_map(
        local_part, mesh=mesh,
        in_specs=(P("dp", None, None), P(None), P("tp", None), P("dp", None)),
        out_specs=(P("dp", None), P("dp", None)), check_vma=False)
```

```python
import functools

import jax
import jax.numpy as jnp
from jax import lax
from jax.experimental import pallas as pl
from jax.experimental.pallas import tpu as pltpu
from jax.sharding import PartitionSpec as P

EPS = 1e-6
LANES = 128
BLOCK = 512
CHUNK = 2 * BLOCK
SLOTS = 7
MESH = pl.DeviceIdType.MESH


def head_kernel(tp, x_hbm, w_ref, e_hbm, ids_ref, out_ref, x_buf, h_buf, e_buf, z_a, z_b,
                idp, m_ref, s_ref, a_ref, p_ref, stats, recv, x_sem, e_sem, send_sem, recv_sem):
    groups, batch, depth = x_hbm.shape
    tokens = groups * batch
    rows = e_hbm.shape[0]
    steps = rows // CHUNK
    width = h_buf.shape[0]
    me = lax.axis_index("tp")

    barrier = pltpu.get_barrier_semaphore()
    x_copy = pltpu.make_async_copy(x_hbm, x_buf, x_sem)
    x_copy.start()

    def e_copy(step, slot):
        first = pl.multiple_of(step * CHUNK, CHUNK)
        return pltpu.make_async_copy(e_hbm.at[pl.ds(first, CHUNK)], e_buf.at[slot], e_sem.at[slot])

    def fill(slot, c):
        e_copy(slot, slot).start()
        return c

    lax.fori_loop(0, SLOTS, fill, 0)
    for k in range(1, tp):
        pl.semaphore_signal(barrier, inc=1, device_id={"tp": lax.rem(me + k, tp)}, device_id_type=MESH)

    idp[...] = jnp.full_like(idp, -1)
    idp[0:batch, 0:groups] = ids_ref[...]
    by_group = jnp.transpose(idp[...])
    sub = lax.broadcasted_iota(jnp.int32, (8, LANES), 0)
    lane = lax.broadcasted_iota(jnp.int32, (8, LANES), 1)
    id_rows = []
    for half in range(width // LANES):
        part = pltpu.roll(by_group[8 * half:8 * half + 8], 0, 1, stride=batch, stride_axis=0)
        part = jnp.where(lane // batch == sub, part, 0)
        id_rows.append(jnp.sum(part, axis=0, keepdims=True))
    id_row = jnp.concatenate(id_rows, axis=1)
    sub_w = lax.broadcasted_iota(jnp.int32, (8, width), 0)
    lane_w = lax.broadcasted_iota(jnp.int32, (8, width), 1)
    wanted = jnp.where(lane_w < tokens, id_row - me * rows - sub_w, -(1 << 30))

    m_ref[...] = jnp.full_like(m_ref, -jnp.inf)
    s_ref[...] = jnp.zeros_like(s_ref)
    a_ref[...] = jnp.zeros_like(a_ref)
    p_ref[...] = jnp.zeros_like(p_ref)

    h_buf[tokens:width, :] = jnp.zeros((width - tokens, depth), h_buf.dtype)
    gain = 1.0 + w_ref[...].astype(jnp.float32)
    x_copy.wait()

    def norm(g, _):
        x = x_buf[g].astype(jnp.float32)
        mean_sq = jnp.sum(x * x, axis=-1, keepdims=True) * (1.0 / depth)
        normed = x * lax.rsqrt(mean_sq + EPS) * gain
        h_buf[pl.ds(pl.multiple_of(g * batch, batch), batch), :] = normed.astype(h_buf.dtype)
        return _

    lax.fori_loop(0, groups, norm, 0)

    def logits(slot, part):
        return lax.dot_general(e_buf[slot, pl.ds(part * BLOCK, BLOCK)], h_buf[...], (((1,), (1,)), ((), ())),
                               preferred_element_type=jnp.float32)

    def fold(z_ref, first):
        z = z_ref[...].reshape(BLOCK // 8, 8, width)
        m_old = m_ref[...]
        m_new = jnp.maximum(m_old, jnp.max(z, axis=0))
        scale = jnp.exp(m_old - m_new)
        e = jnp.exp(z - m_new[None])
        m_ref[...] = m_new
        s_ref[...] = s_ref[...] * scale + jnp.sum(e, axis=0)
        a_ref[...] = a_ref[...] * scale + jnp.sum(e * z, axis=0)
        here = wanted - first
        at = 8 * lax.broadcasted_iota(jnp.int32, z.shape, 0)
        p_ref[...] += jnp.sum(jnp.where(here[None] == at, z, 0.0), axis=0)

    e_copy(0, 0).wait()
    z_a[...] = logits(0, 0)

    def chunk(i, c):
        slot = lax.rem(i, SLOTS)
        z_b[...] = logits(slot, 1)
        fold(z_a, i * CHUNK)

        @pl.when(i + SLOTS < steps)
        def _():
            e_copy(i + SLOTS, slot).start()

        after = lax.rem(i + 1, SLOTS)
        e_copy(i + 1, after).wait()
        z_a[...] = logits(after, 0)
        fold(z_b, i * CHUNK + BLOCK)
        return c

    lax.fori_loop(0, steps - 1, chunk, 0)
    last = (steps - 1) * CHUNK
    z_b[...] = logits((steps - 1) % SLOTS, 1)
    fold(z_a, last)
    fold(z_b, last + BLOCK)

    m8 = m_ref[...]
    m1 = jnp.max(m8, axis=0, keepdims=True)
    c8 = jnp.exp(m8 - m1)
    s1 = jnp.sum(c8 * s_ref[...], axis=0, keepdims=True)
    a1 = jnp.sum(c8 * a_ref[...], axis=0, keepdims=True)
    p1 = jnp.sum(p_ref[...], axis=0, keepdims=True)
    own = jnp.concatenate([m1, s1, a1, p1], axis=0)
    stats[...] = own
    recv[me] = own

    pl.semaphore_wait(barrier, tp - 1)

    def send(k):
        peer = lax.rem(me + k, tp)
        return pltpu.make_async_remote_copy(
            src_ref=stats, dst_ref=recv.at[me], send_sem=send_sem.at[k], recv_sem=recv_sem.at[k],
            device_id={"tp": peer}, device_id_type=MESH)

    for k in range(1, tp):
        send(k).start()
    for k in range(1, tp):
        send(k).wait()

    r = recv[...]
    m = r[:, 0, :]
    top = jnp.max(m, axis=0, keepdims=True)
    c = jnp.exp(m - top)
    total = jnp.sum(c * r[:, 1, :], axis=0, keepdims=True)
    weighted = jnp.sum(c * r[:, 2, :], axis=0, keepdims=True)
    picked = jnp.sum(r[:, 3, :], axis=0, keepdims=True)
    log_norm = top + jnp.log(total)
    log_prob = picked - log_norm
    entropy = log_norm - weighted / total

    out = jnp.zeros((batch, LANES), jnp.float32)
    out_lane = lax.broadcasted_iota(jnp.int32, (batch, LANES), 1)
    row = lax.broadcasted_iota(jnp.int32, (LANES, LANES), 0)
    for half in range(width // LANES):
        cut = slice(half * LANES, (half + 1) * LANES)
        both = jnp.where(row < LANES // 2, log_prob[:, cut], entropy[:, cut])
        col = jnp.transpose(both)
        for j in range(LANES // batch):
            g = half * (LANES // batch) + j
            if g < groups:
                mine = (out_lane == g) | (out_lane == g + LANES // 2)
                out = jnp.where(mine, col[j * batch:(j + 1) * batch], out)
    out_ref[0] = out[:, 0:groups]
    out_ref[1] = out[:, LANES // 2:LANES // 2 + groups]


def solution(mesh):
    tp = mesh.shape["tp"]

    def local_part(hidden, norm_w, embedding, draft_ids):
        batch, groups, depth = hidden.shape
        width = pl.cdiv(batch * groups, 2 * LANES) * 2 * LANES
        x = jnp.transpose(hidden, (1, 0, 2))
        any_space = pl.BlockSpec(memory_space=pl.ANY)
        vmem = pl.BlockSpec(memory_space=pltpu.VMEM)
        out = pl.pallas_call(
            functools.partial(head_kernel, tp),
            out_shape=jax.ShapeDtypeStruct((2, batch, groups), jnp.float32),
            in_specs=[any_space, vmem, any_space, vmem],
            out_specs=vmem,
            scratch_shapes=[
                pltpu.VMEM((groups, batch, depth), hidden.dtype),
                pltpu.VMEM((width, depth), jnp.bfloat16),
                pltpu.VMEM((SLOTS, CHUNK, depth), embedding.dtype),
                pltpu.VMEM((BLOCK, width), jnp.float32),
                pltpu.VMEM((BLOCK, width), jnp.float32),
                pltpu.VMEM((LANES, LANES), jnp.int32),
                pltpu.VMEM((8, width), jnp.float32),
                pltpu.VMEM((8, width), jnp.float32),
                pltpu.VMEM((8, width), jnp.float32),
                pltpu.VMEM((8, width), jnp.float32),
                pltpu.VMEM((4, width), jnp.float32),
                pltpu.VMEM((tp, 4, width), jnp.float32),
                pltpu.SemaphoreType.DMA,
                pltpu.SemaphoreType.DMA((SLOTS,)),
                pltpu.SemaphoreType.DMA((tp,)),
                pltpu.SemaphoreType.DMA((tp,)),
            ],
            compiler_params=pltpu.CompilerParams(
                collective_id=0, has_side_effects=True, vmem_limit_bytes=60 * 1024 * 1024),
        )(x, norm_w.reshape(1, depth), embedding, draft_ids)
        return out[0], out[1]

    return jax.shard_map(
        local_part, mesh=mesh,
        in_specs=(P("dp", None, None), P(None), P("tp", None), P("dp", None)),
        out_specs=(P("dp", None), P("dp", None)), check_vma=False)
```

```python
import functools

import jax
import jax.numpy as jnp
from jax import lax
from jax.experimental import pallas as pl
from jax.experimental.pallas import tpu as pltpu
from jax.sharding import PartitionSpec as P

EPS = 1e-6
LANES = 128
BLOCK = 512
GROUP = 64
CHUNK = 2 * BLOCK
SLOTS = 7
MESH = pl.DeviceIdType.MESH


def head_kernel(tp, x_hbm, w_ref, e_hbm, ids_ref, out_ref, x_buf, h_buf, e_buf, z_a, z_b,
                idp, m_ref, s_ref, a_ref, p_ref, stats, recv, x_sem, e_sem, send_sem, recv_sem):
    groups, batch, depth = x_hbm.shape
    tokens = groups * batch
    rows = e_hbm.shape[0]
    steps = rows // CHUNK
    width = h_buf.shape[0]
    me = lax.axis_index("tp")

    barrier = pltpu.get_barrier_semaphore()
    x_copy = pltpu.make_async_copy(x_hbm, x_buf, x_sem)
    x_copy.start()

    def e_copy(step, slot):
        first = pl.multiple_of(step * CHUNK, CHUNK)
        return pltpu.make_async_copy(e_hbm.at[pl.ds(first, CHUNK)], e_buf.at[slot], e_sem.at[slot])

    def fill(slot, c):
        e_copy(slot, slot).start()
        return c

    lax.fori_loop(0, SLOTS, fill, 0)
    for k in range(1, tp):
        pl.semaphore_signal(barrier, inc=1, device_id={"tp": lax.rem(me + k, tp)}, device_id_type=MESH)

    idp[...] = jnp.full_like(idp, -1)
    idp[0:batch, 0:groups] = ids_ref[...]
    by_group = jnp.transpose(idp[...])
    sub = lax.broadcasted_iota(jnp.int32, (8, LANES), 0)
    lane = lax.broadcasted_iota(jnp.int32, (8, LANES), 1)
    id_rows = []
    for half in range(width // LANES):
        part = pltpu.roll(by_group[8 * half:8 * half + 8], 0, 1, stride=batch, stride_axis=0)
        part = jnp.where(lane // batch == sub, part, 0)
        id_rows.append(jnp.sum(part, axis=0, keepdims=True))
    id_row = jnp.concatenate(id_rows, axis=1)
    sub_w = lax.broadcasted_iota(jnp.int32, (8, width), 0)
    lane_w = lax.broadcasted_iota(jnp.int32, (8, width), 1)
    wanted = jnp.where(lane_w < tokens, id_row - me * rows - sub_w, -(1 << 30))

    m_ref[...] = jnp.full_like(m_ref, -jnp.inf)
    s_ref[...] = jnp.zeros_like(s_ref)
    a_ref[...] = jnp.zeros_like(a_ref)
    p_ref[...] = jnp.zeros_like(p_ref)

    h_buf[tokens:width, :] = jnp.zeros((width - tokens, depth), h_buf.dtype)
    gain = 1.0 + w_ref[...].astype(jnp.float32)
    x_copy.wait()

    def norm(g, _):
        x = x_buf[g].astype(jnp.float32)
        mean_sq = jnp.sum(x * x, axis=-1, keepdims=True) * (1.0 / depth)
        normed = x * lax.rsqrt(mean_sq + EPS) * gain
        h_buf[pl.ds(pl.multiple_of(g * batch, batch), batch), :] = normed.astype(h_buf.dtype)
        return _

    lax.fori_loop(0, groups, norm, 0)

    def logits(slot, part):
        return lax.dot_general(e_buf[slot, pl.ds(part * BLOCK, BLOCK)], h_buf[...], (((1,), (1,)), ((), ())),
                               preferred_element_type=jnp.float32)

    def fold(z_ref, first):
        m, total, weighted, pick = m_ref[...], s_ref[...], a_ref[...], p_ref[...]
        for group in range(BLOCK // GROUP):
            z = z_ref[group * GROUP:(group + 1) * GROUP, :].reshape(GROUP // 8, 8, width)
            m_new = jnp.maximum(m, jnp.max(z, axis=0))
            scale = jnp.exp(m - m_new)
            e = jnp.exp(z - m_new[None])
            m = m_new
            total = total * scale + jnp.sum(e, axis=0)
            weighted = weighted * scale + jnp.sum(e * z, axis=0)
            here = wanted - (first + group * GROUP)
            for r in range(GROUP // 8):
                pick = jnp.where(here == 8 * r, z[r], pick)
        m_ref[...], s_ref[...], a_ref[...], p_ref[...] = m, total, weighted, pick

    e_copy(0, 0).wait()
    z_a[...] = logits(0, 0)

    def chunk(i, c):
        slot = lax.rem(i, SLOTS)
        z_b[...] = logits(slot, 1)
        fold(z_a, i * CHUNK)

        @pl.when(i + SLOTS < steps)
        def _():
            e_copy(i + SLOTS, slot).start()

        after = lax.rem(i + 1, SLOTS)
        e_copy(i + 1, after).wait()
        z_a[...] = logits(after, 0)
        fold(z_b, i * CHUNK + BLOCK)
        return c

    lax.fori_loop(0, steps - 1, chunk, 0)
    last = (steps - 1) * CHUNK
    z_b[...] = logits((steps - 1) % SLOTS, 1)
    fold(z_a, last)
    fold(z_b, last + BLOCK)

    m8 = m_ref[...]
    m1 = jnp.max(m8, axis=0, keepdims=True)
    c8 = jnp.exp(m8 - m1)
    s1 = jnp.sum(c8 * s_ref[...], axis=0, keepdims=True)
    a1 = jnp.sum(c8 * a_ref[...], axis=0, keepdims=True)
    p1 = jnp.sum(p_ref[...], axis=0, keepdims=True)
    own = jnp.concatenate([m1, s1, a1, p1], axis=0)
    stats[...] = own
    recv[me] = own

    pl.semaphore_wait(barrier, tp - 1)

    def send(k):
        peer = lax.rem(me + k, tp)
        return pltpu.make_async_remote_copy(
            src_ref=stats, dst_ref=recv.at[me], send_sem=send_sem.at[k], recv_sem=recv_sem.at[k],
            device_id={"tp": peer}, device_id_type=MESH)

    for k in range(1, tp):
        send(k).start()
    for k in range(1, tp):
        send(k).wait()

    r = recv[...]
    m = r[:, 0, :]
    top = jnp.max(m, axis=0, keepdims=True)
    c = jnp.exp(m - top)
    total = jnp.sum(c * r[:, 1, :], axis=0, keepdims=True)
    weighted = jnp.sum(c * r[:, 2, :], axis=0, keepdims=True)
    picked = jnp.sum(r[:, 3, :], axis=0, keepdims=True)
    log_norm = top + jnp.log(total)
    log_prob = picked - log_norm
    entropy = log_norm - weighted / total

    out = jnp.zeros((batch, LANES), jnp.float32)
    out_lane = lax.broadcasted_iota(jnp.int32, (batch, LANES), 1)
    row = lax.broadcasted_iota(jnp.int32, (LANES, LANES), 0)
    for half in range(width // LANES):
        cut = slice(half * LANES, (half + 1) * LANES)
        both = jnp.where(row < LANES // 2, log_prob[:, cut], entropy[:, cut])
        col = jnp.transpose(both)
        for j in range(LANES // batch):
            g = half * (LANES // batch) + j
            if g < groups:
                mine = (out_lane == g) | (out_lane == g + LANES // 2)
                out = jnp.where(mine, col[j * batch:(j + 1) * batch], out)
    out_ref[0] = out[:, 0:groups]
    out_ref[1] = out[:, LANES // 2:LANES // 2 + groups]


def solution(mesh):
    tp = mesh.shape["tp"]

    def local_part(hidden, norm_w, embedding, draft_ids):
        batch, groups, depth = hidden.shape
        width = pl.cdiv(batch * groups, 2 * LANES) * 2 * LANES
        x = jnp.transpose(hidden, (1, 0, 2))
        any_space = pl.BlockSpec(memory_space=pl.ANY)
        vmem = pl.BlockSpec(memory_space=pltpu.VMEM)
        out = pl.pallas_call(
            functools.partial(head_kernel, tp),
            out_shape=jax.ShapeDtypeStruct((2, batch, groups), jnp.float32),
            in_specs=[any_space, vmem, any_space, vmem],
            out_specs=vmem,
            scratch_shapes=[
                pltpu.VMEM((groups, batch, depth), hidden.dtype),
                pltpu.VMEM((width, depth), jnp.bfloat16),
                pltpu.VMEM((SLOTS, CHUNK, depth), embedding.dtype),
                pltpu.VMEM((BLOCK, width), jnp.float32),
                pltpu.VMEM((BLOCK, width), jnp.float32),
                pltpu.VMEM((LANES, LANES), jnp.int32),
                pltpu.VMEM((8, width), jnp.float32),
                pltpu.VMEM((8, width), jnp.float32),
                pltpu.VMEM((8, width), jnp.float32),
                pltpu.VMEM((8, width), jnp.float32),
                pltpu.VMEM((4, width), jnp.float32),
                pltpu.VMEM((tp, 4, width), jnp.float32),
                pltpu.SemaphoreType.DMA,
                pltpu.SemaphoreType.DMA((SLOTS,)),
                pltpu.SemaphoreType.DMA((tp,)),
                pltpu.SemaphoreType.DMA((tp,)),
            ],
            compiler_params=pltpu.CompilerParams(
                collective_id=0, has_side_effects=True, vmem_limit_bytes=60 * 1024 * 1024),
        )(x, norm_w.reshape(1, depth), embedding, draft_ids)
        return out[0], out[1]

    return jax.shard_map(
        local_part, mesh=mesh,
        in_specs=(P("dp", None, None), P(None), P("tp", None), P("dp", None)),
        out_specs=(P("dp", None), P("dp", None)), check_vma=False)
```
